32 devices in a mesh: rep: 2 (over x), model: 4 (over z), vocab: 4 (over y, core).
Axes of the slice: x: 2, y: 2, z: 4, core: 2. Of those that a mesh axis runs over, the one named last changes fastest.
Arguments:
- hidden: bfloat16 [1024, 4096], P(('rep', 'model', 'vocab')), parts along dimension 0
- head_rows: bfloat16 [128256, 4096], P(('model', 'vocab'))
- allowed_ids: int32 [1024, 32], P(('rep', 'model', 'vocab')), parts along dimension 0
- valid_mask: int32 [1024, 32], P(('rep', 'model', 'vocab')), parts along dimension 0
- target_pos: int32 [1024], P(('rep', 'model', 'vocab')), parts along dimension 0
Outputs:
- output 1: float32 [1024, 32], P(('rep', 'model', 'vocab')), parts along dimension 0
- output 2: float32 [1024], P(('rep', 'model', 'vocab')), parts along dimension 0
There are 2 independent parts. The reference program is written for one: setup_inputs(seed, part) draws one part's arguments, and reference() takes and returns one part's arrays. A program takes and returns all parts, laid end to end along the dimension named above; an argument that names none is the same for every part.
All inputs are finite; a program needn't handle non-finite values.
Results may differ from the reference program's by a relative error of at most 0.001.
Values are sent between devices in bfloat16 or wider.
A program may use at most 1 GiB of HBM per device.

```python
import jax
import jax.numpy as jnp
from jax import lax

VOCAB_SIZE = 128256
MODEL_WIDTH = 4096
NUM_ROWS = 512
LIST_LEN = 32
NUM_SHARDS = 16
OWNER_RUNS = 4
TEMPERATURE = 0.5


def draw_lists(idx_key):
    shard_len = VOCAB_SIZE // NUM_SHARDS
    run_len = LIST_LEN // OWNER_RUNS
    key_rot, key_step, key_start, key_count, key_target = jax.random.split(idx_key, 5)
    rotation = jax.random.randint(key_rot, (NUM_ROWS, 1), 0, NUM_SHARDS - 1)
    run_index = jnp.arange(OWNER_RUNS)[None, :]
    owners = jnp.where(run_index == 0, 0, 1 + (rotation + run_index - 1) % (NUM_SHARDS - 1))
    stride = jax.random.randint(key_step, (NUM_ROWS, OWNER_RUNS), 1, shard_len // run_len + 1)
    run_start = jax.random.randint(key_start, (NUM_ROWS, OWNER_RUNS), 0, shard_len - stride * (run_len - 1))
    offsets = run_start[:, :, None] + stride[:, :, None] * jnp.arange(run_len)[None, None, :]
    allowed_ids = (owners[:, :, None] * shard_len + offsets).reshape(NUM_ROWS, LIST_LEN).astype(jnp.int32)
    counts = LIST_LEN - jax.random.randint(key_count, (NUM_ROWS,), 0, LIST_LEN // 2)
    counts = jnp.where(jnp.arange(NUM_ROWS) == 0, LIST_LEN, counts)
    valid_mask = (jnp.arange(LIST_LEN)[None, :] < counts[:, None]).astype(jnp.int32)
    target_pos = jax.random.randint(key_target, (NUM_ROWS,), 0, counts).astype(jnp.int32)
    return allowed_ids, valid_mask, target_pos


def setup_inputs(seed: int = 0, part: int = 0) -> dict:
    base_key = jax.random.key(seed)
    part_key = jax.random.fold_in(base_key, part)
    key_hidden, key_lists = jax.random.split(part_key, 2)
    hidden = jax.random.normal(key_hidden, (NUM_ROWS, MODEL_WIDTH), jnp.float32).astype(jnp.bfloat16)
    head_rows = (jax.random.normal(jax.random.key(seed + 1), (VOCAB_SIZE, MODEL_WIDTH), jnp.float32) * MODEL_WIDTH ** -0.5).astype(jnp.bfloat16)
    allowed_ids, valid_mask, target_pos = draw_lists(key_lists)
    return {'hidden': hidden, 'head_rows': head_rows, 'allowed_ids': allowed_ids, 'valid_mask': valid_mask, 'target_pos': target_pos}


def reference(hidden, head_rows, allowed_ids, valid_mask, target_pos):
    def row_scores(row_args):
        h_row, row_ids = row_args
        return jnp.dot(head_rows[row_ids], h_row, preferred_element_type=jnp.float32)

    scores = lax.map(row_scores, (hidden, allowed_ids)) / TEMPERATURE
    is_valid = valid_mask > 0
    scores = jnp.where(is_valid, scores, -jnp.inf)
    top_score = jnp.max(scores, axis=1, keepdims=True)
    log_norm = top_score[:, 0] + jnp.log(jnp.sum(jnp.exp(scores - top_score), axis=1))
    probs = jnp.where(is_valid, jnp.exp(scores - log_norm[:, None]), 0.0)
    picked_score = jnp.take_along_axis(scores, target_pos[:, None], axis=1)[:, 0]
    return probs, picked_score - log_norm
```

```python
import functools

import jax
import jax.numpy as jnp
from jax import lax
from jax.experimental import pallas as pl
from jax.experimental.pallas import tpu as pltpu
from jax.sharding import PartitionSpec as P

TEMPERATURE = 0.5
MESH = pl.DeviceIdType.MESH
CONTRACT_LAST = (((1,), (1,)), ((), ()))
NUM_SHARDS = 16
NUM_PIECES = 8
NUM_SLOTS = 6
HEAD_BLOCK = 1008
SLOT_CAP = 8
LANES = 128
LEAD = 3


def kernel(shard_len, width, rows,
           tgt_ref, ids_ref, valid_ref, hidden_ref, head_ref,
           p_ref, lp_ref,
           head_buf, h_buf, square, turned, codes, offs_out, offs_in, acc, ret_in,
           head_sem, local_sem, recv_sem, own_sem, far_sem, relay_sem, hop_sem,
           offs_send, offs_recv, ret_send, ret_recv):
    depth = width // NUM_PIECES
    half = NUM_SHARDS // 2 * rows
    num_phases = 2 * NUM_PIECES
    z, v = lax.axis_index('model'), lax.axis_index('vocab')
    me = z * 4 + v
    z_near = z + 1 - 2 * lax.rem(z, 2)
    z_far = 2 * lax.rem(lax.div(z, 2) + 1, 2)
    v_other = lax.rem(v + 2, 4)
    v_sib = v + 1 - 2 * lax.rem(v, 2)
    v_sib_other = lax.rem(v_sib + 2, 4)

    def partner(step):
        return lax.rem(me + step, NUM_SHARDS)

    def device(shard):
        return {'model': lax.div(shard, 4), 'vocab': lax.rem(shard, 4)}

    barrier = pltpu.get_barrier_semaphore()
    for step in range(1, NUM_SHARDS):
        pl.semaphore_signal(barrier, inc=1, device_id=device(partner(step)), device_id_type=MESH)

    blocks = [(start, min(HEAD_BLOCK, shard_len - start)) for start in range(0, shard_len, HEAD_BLOCK)]

    def piece_of(phase):
        return lax.rem(phase + 2 * lax.div(phase, NUM_PIECES), NUM_PIECES)

    def head_copies(phase):
        cols = pl.ds(pl.multiple_of(piece_of(phase) * depth, depth), depth)
        slot = lax.rem(phase, NUM_SLOTS)
        return [pltpu.make_async_copy(head_ref.at[pl.ds(start, size), cols],
                                      head_buf.at[slot, pl.ds(start, size), :], head_sem.at[slot, i])
                for i, (start, size) in enumerate(blocks)]

    def block_of(shard, piece):
        return h_buf.at[piece, pl.ds(pl.multiple_of(shard * rows, rows), rows), :]

    local_copies = [pltpu.make_async_copy(hidden_ref.at[:, pl.ds(k * depth, depth)], block_of(me, k), local_sem.at[k])
                    for k in range(NUM_PIECES)]
    for copy in local_copies:
        copy.start()
    for phase in range(NUM_SLOTS):
        for copy in head_copies(phase):
            copy.start()

    square[...] = jnp.zeros_like(square)
    masked_ids = jnp.where(valid_ref[...] > 0, ids_ref[...], -1)
    for group in range(4):
        square[rows * group:rows * group + rows, 0:32] = masked_ids
    ids_t = jnp.transpose(square[...])[0:32, :]
    owner = jnp.zeros_like(ids_t)
    for s in range(1, NUM_SHARDS):
        owner = owner + jnp.where(ids_t >= s * shard_len, 1, 0)
    lane = lax.broadcasted_iota(jnp.int32, (32, LANES), 1)
    list_pos = lax.broadcasted_iota(jnp.int32, (32, LANES), 0)
    mine = (lane >= v * rows) & (lane < v * rows + rows) & (ids_t >= 0)
    owner = jnp.where(mine, owner, -1)
    offset1 = ids_t - owner * shard_len + 1
    rank = jnp.zeros_like(owner)
    for i in range(31):
        rank = rank + jnp.where((owner == owner[i:i + 1, :]) & (list_pos > i), 1, 0)
    code = jnp.where(mine, owner * SLOT_CAP + rank, -1)
    codes[0, :, :] = owner
    codes[1, :, :] = jnp.minimum(rank, SLOT_CAP - 1)
    slot_pos = lax.broadcasted_iota(jnp.int32, (SLOT_CAP, LANES), 0)
    tiles = [jnp.zeros((SLOT_CAP, LANES), jnp.int32) for _ in range(NUM_SHARDS)]
    for j in range(32):
        code_j, offset_j = code[j:j + 1, :], offset1[j:j + 1, :]
        for s in range(NUM_SHARDS):
            tiles[s] = jnp.where(code_j == slot_pos + s * SLOT_CAP, offset_j, tiles[s])
    for s in range(NUM_SHARDS):
        offs_out[s, :, :] = tiles[s]
    offs_in[me, :, :] = offs_out[me, :, :]
    acc[...] = jnp.zeros_like(acc)

    for copy in local_copies:
        copy.wait()
    pl.semaphore_wait(barrier, NUM_SHARDS - 1)

    def send_block(shard, piece, send_sem, to_z, to_v):
        return pltpu.make_async_remote_copy(
            src_ref=block_of(shard, piece), dst_ref=block_of(shard, piece), send_sem=send_sem,
            recv_sem=recv_sem.at[shard, piece], device_id={'model': to_z, 'vocab': to_v}, device_id_type=MESH)

    def arrived(shard, piece):
        send_block(shard, piece, recv_sem.at[shard, piece], z, v_sib).wait_recv()

    def own_sends(k):
        return [send_block(me, k, own_sem.at[0, k], z_near, v),
                send_block(me, k, own_sem.at[1, k], z, v_other),
                send_block(me, k, own_sem.at[2, k], z, v_sib)]

    def far_sends(k):
        return [send_block(me, k, far_sem.at[e, k], z_far + e, v) for e in range(2)]

    def send_offs(step):
        to = partner(step)
        return pltpu.make_async_remote_copy(
            src_ref=offs_out.at[to], dst_ref=offs_in.at[me], send_sem=offs_send.at[step], recv_sem=offs_recv.at[me],
            device_id=device(to), device_id_type=MESH)

    def pair_base(phase):
        return 2 * lax.rem(lax.div(z, 2) + lax.div(phase, NUM_PIECES), 2)

    def relay_sends(phase, e):
        shard, k = (pair_base(phase) + e) * 4 + v, piece_of(phase)
        return [send_block(shard, k, relay_sem.at[0, e, phase], z, v_other),
                send_block(shard, k, relay_sem.at[1, e, phase], z, v_sib)]

    def relay(phase):
        for e in range(2):
            @pl.when((phase < num_phases) & (pair_base(phase) + e != z))
            def _():
                arrived((pair_base(phase) + e) * 4 + v, piece_of(phase))
                for copy in relay_sends(phase, e):
                    copy.start()

    def hop_send(phase, e):
        return send_block((pair_base(phase) + e) * 4 + v_other, piece_of(phase), hop_sem.at[e, phase], z, v_sib)

    def hop(phase):
        @pl.when(phase < num_phases)
        def _():
            for e in range(2):
                arrived((pair_base(phase) + e) * 4 + v_other, piece_of(phase))
                hop_send(phase, e).start()

    def settle(phase):
        for e in range(2):
            arrived((pair_base(phase) + e) * 4 + v_sib, piece_of(phase))
            arrived((pair_base(phase) + e) * 4 + v_sib_other, piece_of(phase))

    def send_scores(step):
        to = partner(step)
        return pltpu.make_async_remote_copy(
            src_ref=acc.at[lax.div(to, 4)], dst_ref=ret_in.at[me], send_sem=ret_send.at[step], recv_sem=ret_recv.at[me],
            device_id=device(to), device_id_type=MESH)

    def near(step):
        return lax.div(partner(step), 8) == lax.div(me, 8)

    for copy in own_sends(0):
        copy.start()
    for step in range(1, NUM_SHARDS):
        send_offs(step).start()
    for k in range(1, NUM_PIECES):
        for copy in own_sends(k):
            copy.start()
    for phase in range(LEAD):
        relay(phase)
    hop(0)

    def wait_offs(step):
        src = partner(step)
        pltpu.make_async_remote_copy(
            src_ref=offs_out.at[src], dst_ref=offs_in.at[src], send_sem=offs_send.at[step], recv_sem=offs_recv.at[src],
            device_id=device(src), device_id_type=MESH).wait_recv()

    for step in range(1, NUM_SHARDS):
        wait_offs(step)

    def run_phase(phase, carry):
        @pl.when(phase < NUM_PIECES)
        def _():
            for copy in far_sends(piece_of(phase + NUM_PIECES)):
                copy.start()

        relay(phase + LEAD)
        hop(phase + 1)
        settle(phase)

        @pl.when((phase < NUM_PIECES) | (phase >= NUM_PIECES + NUM_SLOTS))
        def _():
            for copy in head_copies(phase):
                copy.wait()

        slot = lax.rem(phase, NUM_SLOTS)
        base = pair_base(phase)
        hidden = h_buf[piece_of(phase), pl.ds(pl.multiple_of(base * 4 * rows, half), half), :]
        offsets = []
        for l in range(2):
            total = offs_in[(base + l) * 4, :, :]
            for u in range(1, 4):
                total = total + offs_in[(base + l) * 4 + u, :, :]
            offsets.append(total - 1)
        sums = [acc[base + l, :, :] for l in range(2)]
        for start, size in blocks:
            scores = lax.dot_general(head_buf[slot, start:start + size, :], hidden, CONTRACT_LAST,
                                     preferred_element_type=jnp.float32)
            for l in range(2):
                low = offsets[l] & 7
                high = (offsets[l] >> 3) - start // 8
                found = jnp.zeros((SLOT_CAP, LANES), jnp.float32)
                for g in range(size // 8):
                    tile = scores[8 * g:8 * g + 8, LANES * l:LANES * l + LANES]
                    found = jnp.where(high == g, jnp.take_along_axis(tile, low, axis=0), found)
                sums[l] = sums[l] + found
        for l in range(2):
            acc[base + l, :, :] = sums[l]

        @pl.when((phase < NUM_PIECES - NUM_SLOTS) | ((phase >= NUM_PIECES) & (phase < 2 * NUM_PIECES - NUM_SLOTS)))
        def _():
            for copy in head_copies(phase + NUM_SLOTS):
                copy.start()

        @pl.when(phase == NUM_PIECES)
        def _():
            for step in range(1, NUM_SHARDS):
                @pl.when(near(step))
                def _():
                    send_scores(step).start()

        return carry

    lax.fori_loop(0, num_phases, run_phase, 0)

    for step in range(1, NUM_SHARDS):
        @pl.when(jnp.logical_not(near(step)))
        def _():
            send_scores(step).start()
    ret_in[me, :, :] = acc[z, :, :]

    row_pos = lax.broadcasted_iota(jnp.int32, (rows, 32), 0)
    target = jnp.zeros((rows, 32), jnp.int32)
    for b in range(rows):
        target = jnp.where(row_pos == b, tgt_ref[b], target)

    def end_piece(k, carry):
        for copy in own_sends(k) + far_sends(k):
            copy.wait_send()
        return carry

    lax.fori_loop(0, NUM_PIECES, end_piece, 0)

    def end_phase(phase, carry):
        for e in range(2):
            @pl.when(pair_base(phase) + e != z)
            def _():
                for copy in relay_sends(phase, e):
                    copy.wait_send()
            hop_send(phase, e).wait_send()
        return carry

    lax.fori_loop(0, num_phases, end_phase, 0)
    for step in range(1, NUM_SHARDS):
        send_offs(step).wait_send()
        send_scores(step).wait_send()
    for step in range(1, NUM_SHARDS):
        src = partner(step)
        pltpu.make_async_remote_copy(
            src_ref=acc.at[0], dst_ref=ret_in.at[src], send_sem=ret_send.at[step], recv_sem=ret_recv.at[src],
            device_id=device(src), device_id_type=MESH).wait_recv()

    turned[...] = jnp.zeros_like(turned)
    for q in range(4):
        owner_q, rank_q = codes[0, 8 * q:8 * q + 8, :], codes[1, 8 * q:8 * q + 8, :]
        picked = jnp.zeros((8, LANES), jnp.float32)
        for s in range(NUM_SHARDS):
            picked = jnp.where(owner_q == s, jnp.take_along_axis(ret_in[s, :, :], rank_q, axis=0), picked)
        turned[8 * q:8 * q + 8, :] = picked
    turned[...] = jnp.transpose(turned[...])
    raw = turned[pl.ds(pl.multiple_of(v * rows, rows), rows), :][:, 0:32]
    is_valid = valid_ref[...] > 0
    logits = jnp.where(is_valid, raw / TEMPERATURE, -jnp.inf)
    top = jnp.max(logits, axis=1, keepdims=True)
    log_norm = top + jnp.log(jnp.sum(jnp.exp(logits - top), axis=1, keepdims=True))
    p_ref[...] = jnp.where(is_valid, jnp.exp(logits - log_norm), 0.0)
    col_pos = lax.broadcasted_iota(jnp.int32, (rows, 32), 1)
    chosen = jnp.sum(jnp.where(col_pos == target, logits, 0.0), axis=1, keepdims=True)
    turned[0:rows, :] = jnp.broadcast_to(chosen - log_norm, (rows, LANES))
    lp_ref[...] = jnp.transpose(turned[...])[0:1, 0:rows]


def solution(mesh):
    shard_axes = ('model', 'vocab')
    row_spec = P(('rep', 'model', 'vocab'), None)
    vec_spec = P(('rep', 'model', 'vocab'))

    def local_step(hidden, head_rows, allowed_ids, valid_mask, target_pos):
        rows, width = hidden.shape
        shard_len = head_rows.shape[0]
        depth = width // NUM_PIECES
        num_blocks = -(-shard_len // HEAD_BLOCK)
        dma = pltpu.SemaphoreType.DMA
        tile = (SLOT_CAP, LANES)
        p, lp = pl.pallas_call(
            functools.partial(kernel, shard_len, width, rows),
            out_shape=(jax.ShapeDtypeStruct((rows, 32), jnp.float32), jax.ShapeDtypeStruct((1, rows), jnp.float32)),
            in_specs=[pl.BlockSpec(memory_space=pltpu.SMEM), pl.BlockSpec(memory_space=pltpu.VMEM),
                      pl.BlockSpec(memory_space=pltpu.VMEM), pl.BlockSpec(memory_space=pl.ANY),
                      pl.BlockSpec(memory_space=pl.ANY)],
            out_specs=(pl.BlockSpec(memory_space=pltpu.VMEM), pl.BlockSpec(memory_space=pltpu.VMEM)),
            scratch_shapes=[
                pltpu.VMEM((NUM_SLOTS, shard_len, depth), jnp.bfloat16),
                pltpu.VMEM((NUM_PIECES, NUM_SHARDS * rows, depth), jnp.bfloat16),
                pltpu.VMEM((LANES, LANES), jnp.int32),
                pltpu.VMEM((LANES, LANES), jnp.float32),
                pltpu.VMEM((2, 32, LANES), jnp.int32),
                pltpu.VMEM((NUM_SHARDS,) + tile, jnp.int32),
                pltpu.VMEM((NUM_SHARDS,) + tile, jnp.int32),
                pltpu.VMEM((4,) + tile, jnp.float32),
                pltpu.VMEM((NUM_SHARDS,) + tile, jnp.float32),
                dma((NUM_SLOTS, num_blocks)), dma((NUM_PIECES,)), dma((NUM_SHARDS, NUM_PIECES)),
                dma((3, NUM_PIECES)), dma((2, NUM_PIECES)), dma((2, 2, 2 * NUM_PIECES)), dma((2, 2 * NUM_PIECES)),
                dma((NUM_SHARDS,)), dma((NUM_SHARDS,)), dma((NUM_SHARDS,)), dma((NUM_SHARDS,)),
            ],
            compiler_params=pltpu.CompilerParams(collective_id=0, has_side_effects=True, vmem_limit_bytes=67043328),
        )(target_pos, allowed_ids, valid_mask, hidden, head_rows)
        return p, lp.reshape(rows)

    return jax.shard_map(local_step, mesh=mesh, in_specs=(row_spec, P(shard_axes, None), row_spec, row_spec, vec_spec),
                         out_specs=(row_spec, vec_spec), check_vma=False)
```

```python
import functools

import jax
import jax.numpy as jnp
from jax import lax
from jax.experimental import pallas as pl
from jax.experimental.pallas import tpu as pltpu
from jax.sharding import PartitionSpec as P

TEMPERATURE = 0.5
MESH = pl.DeviceIdType.MESH
CONTRACT_LAST = (((1,), (1,)), ((), ()))
NUM_SHARDS = 16
NUM_PIECES = 8
NUM_SLOTS = 6
HEAD_BLOCK = 1008
SLOT_CAP = 8
LANES = 128
LEAD = 3


def kernel(shard_len, width, rows,
           tgt_hbm, ids_hbm, valid_hbm, hidden_ref, head_ref,
           p_hbm, lp_hbm,
           tgt_ref, ids_ref, valid_ref, p_ref, lp_ref, small_sem,
           head_buf, h_buf, square, turned, codes, offs_out, offs_in, acc, ret_in,
           head_sem, local_sem, recv_sem, own_sem, far_sem, relay_sem, hop_sem,
           offs_send, offs_recv, ret_send, ret_recv):
    depth = width // NUM_PIECES
    half = NUM_SHARDS // 2 * rows
    num_phases = 2 * NUM_PIECES
    z, v = lax.axis_index('model'), lax.axis_index('vocab')
    me = z * 4 + v
    z_near = z + 1 - 2 * lax.rem(z, 2)
    z_far = 2 * lax.rem(lax.div(z, 2) + 1, 2)
    v_other = lax.rem(v + 2, 4)
    v_sib = v + 1 - 2 * lax.rem(v, 2)
    v_sib_other = lax.rem(v_sib + 2, 4)

    def partner(step):
        return lax.rem(me + step, NUM_SHARDS)

    def device(shard):
        return {'model': lax.div(shard, 4), 'vocab': lax.rem(shard, 4)}

    barrier = pltpu.get_barrier_semaphore()
    for step in range(1, NUM_SHARDS):
        pl.semaphore_signal(barrier, inc=1, device_id=device(partner(step)), device_id_type=MESH)

    blocks = [(start, min(HEAD_BLOCK, shard_len - start)) for start in range(0, shard_len, HEAD_BLOCK)]

    def piece_of(phase):
        return lax.rem(phase + 2 * lax.div(phase, NUM_PIECES), NUM_PIECES)

    def head_copies(phase):
        cols = pl.ds(pl.multiple_of(piece_of(phase) * depth, depth), depth)
        slot = lax.rem(phase, NUM_SLOTS)
        return [pltpu.make_async_copy(head_ref.at[pl.ds(start, size), cols],
                                      head_buf.at[slot, pl.ds(start, size), :], head_sem.at[slot, i])
                for i, (start, size) in enumerate(blocks)]

    def block_of(shard, piece):
        return h_buf.at[piece, pl.ds(pl.multiple_of(shard * rows, rows), rows), :]

    local_copies = [pltpu.make_async_copy(hidden_ref.at[:, pl.ds(k * depth, depth)], block_of(me, k), local_sem.at[k])
                    for k in range(NUM_PIECES)]
    small_copies = [pltpu.make_async_copy(src, dst, small_sem.at[i]) for i, (src, dst) in enumerate(
        ((ids_hbm, ids_ref), (valid_hbm, valid_ref), (tgt_hbm, tgt_ref)))]
    out_copies = [pltpu.make_async_copy(src, dst, small_sem.at[3 + i]) for i, (src, dst) in enumerate(
        ((p_ref, p_hbm), (lp_ref, lp_hbm)))]
    for copy in local_copies[:LEAD] + small_copies + local_copies[LEAD:]:
        copy.start()
    for phase in range(NUM_SLOTS):
        for copy in head_copies(phase):
            copy.start(priority=1)

    pl.semaphore_wait(barrier, NUM_SHARDS - 1)

    def send_block(shard, piece, send_sem, to_z, to_v):
        return pltpu.make_async_remote_copy(
            src_ref=block_of(shard, piece), dst_ref=block_of(shard, piece), send_sem=send_sem,
            recv_sem=recv_sem.at[shard, piece], device_id={'model': to_z, 'vocab': to_v}, device_id_type=MESH)

    def arrived(shard, piece):
        send_block(shard, piece, recv_sem.at[shard, piece], z, v_sib).wait_recv()

    def line_send(k):
        return send_block(me, k, own_sem.at[0, k], z_near, v)

    def side_sends(k):
        return [send_block(me, k, own_sem.at[1, k], z, v_other), send_block(me, k, own_sem.at[2, k], z, v_sib)]

    def far_sends(k):
        return [send_block(me, k, far_sem.at[e, k], z_far + e, v) for e in range(2)]

    def send_offs(step):
        to = partner(step)
        return pltpu.make_async_remote_copy(
            src_ref=offs_out.at[to], dst_ref=offs_in.at[me], send_sem=offs_send.at[step], recv_sem=offs_recv.at[me],
            device_id=device(to), device_id_type=MESH)

    def pair_base(phase):
        return 2 * lax.rem(lax.div(z, 2) + lax.div(phase, NUM_PIECES), 2)

    def relay_sends(phase, e):
        shard, k = (pair_base(phase) + e) * 4 + v, piece_of(phase)
        return [send_block(shard, k, relay_sem.at[0, e, phase], z, v_other),
                send_block(shard, k, relay_sem.at[1, e, phase], z, v_sib)]

    def relay(phase):
        for e in range(2):
            @pl.when((phase < num_phases) & (pair_base(phase) + e != z))
            def _():
                arrived((pair_base(phase) + e) * 4 + v, piece_of(phase))
                for copy in relay_sends(phase, e):
                    copy.start()

    def hop_send(phase, e):
        return send_block((pair_base(phase) + e) * 4 + v_other, piece_of(phase), hop_sem.at[e, phase], z, v_sib)

    def hop(phase):
        @pl.when(phase < num_phases)
        def _():
            for e in range(2):
                arrived((pair_base(phase) + e) * 4 + v_other, piece_of(phase))
                hop_send(phase, e).start()

    def settle(phase):
        for e in range(2):
            arrived((pair_base(phase) + e) * 4 + v_sib, piece_of(phase))
            arrived((pair_base(phase) + e) * 4 + v_sib_other, piece_of(phase))

    def send_scores(step):
        to = partner(step)
        return pltpu.make_async_remote_copy(
            src_ref=acc.at[lax.div(to, 4)], dst_ref=ret_in.at[me], send_sem=ret_send.at[step], recv_sem=ret_recv.at[me],
            device_id=device(to), device_id_type=MESH)

    def near(step):
        return lax.div(partner(step), 8) == lax.div(me, 8)

    for k in range(LEAD):
        local_copies[k].wait()
        line_send(k).start()
        for copy in side_sends(k):
            copy.start()
    for copy in small_copies:
        copy.wait()

    square[...] = jnp.zeros_like(square)
    masked_ids = jnp.where(valid_ref[...] > 0, ids_ref[...], -1)
    for group in range(4):
        square[rows * group:rows * group + rows, 0:32] = masked_ids
    ids_t = jnp.transpose(square[...])[0:32, :]
    owner = jnp.zeros_like(ids_t)
    for s in range(1, NUM_SHARDS):
        owner = owner + jnp.where(ids_t >= s * shard_len, 1, 0)
    lane = lax.broadcasted_iota(jnp.int32, (32, LANES), 1)
    list_pos = lax.broadcasted_iota(jnp.int32, (32, LANES), 0)
    mine = (lane >= v * rows) & (lane < v * rows + rows) & (ids_t >= 0)
    owner = jnp.where(mine, owner, -1)
    offset1 = ids_t - owner * shard_len + 1
    rank = jnp.zeros_like(owner)
    for i in range(31):
        rank = rank + jnp.where((owner == owner[i:i + 1, :]) & (list_pos > i), 1, 0)
    code = jnp.where(mine, owner * SLOT_CAP + rank, -1)
    codes[0, :, :] = owner
    codes[1, :, :] = jnp.minimum(rank, SLOT_CAP - 1)
    slot_pos = lax.broadcasted_iota(jnp.int32, (SLOT_CAP, LANES), 0)
    tiles = [jnp.zeros((SLOT_CAP, LANES), jnp.int32) for _ in range(NUM_SHARDS)]
    for j in range(32):
        code_j, offset_j = code[j:j + 1, :], offset1[j:j + 1, :]
        for s in range(NUM_SHARDS):
            tiles[s] = jnp.where(code_j == slot_pos + s * SLOT_CAP, offset_j, tiles[s])
    for s in range(NUM_SHARDS):
        offs_out[s, :, :] = tiles[s]
    offs_in[me, :, :] = offs_out[me, :, :]
    acc[...] = jnp.zeros_like(acc)

    for step in range(1, NUM_SHARDS):
        send_offs(step).start()
    for k in range(LEAD, NUM_PIECES):
        local_copies[k].wait()
        line_send(k).start()
    for phase in range(LEAD):
        relay(phase)
        for copy in side_sends(LEAD + phase):
            copy.start()
    hop(0)

    def wait_offs(step):
        src = partner(step)
        pltpu.make_async_remote_copy(
            src_ref=offs_out.at[src], dst_ref=offs_in.at[src], send_sem=offs_send.at[step], recv_sem=offs_recv.at[src],
            device_id=device(src), device_id_type=MESH).wait_recv()

    for step in range(1, NUM_SHARDS):
        wait_offs(step)

    def run_phase(phase, carry):
        @pl.when(phase < NUM_PIECES)
        def _():
            for copy in far_sends(piece_of(phase + NUM_PIECES)):
                copy.start()

        relay(phase + LEAD)

        @pl.when(phase < NUM_PIECES - 2 * LEAD)
        def _():
            for copy in side_sends(phase + 2 * LEAD):
                copy.start()

        hop(phase + 1)
        settle(phase)

        @pl.when((phase < NUM_PIECES) | (phase >= NUM_PIECES + NUM_SLOTS))
        def _():
            for copy in head_copies(phase):
                copy.wait()

        slot = lax.rem(phase, NUM_SLOTS)
        base = pair_base(phase)
        hidden = h_buf[piece_of(phase), pl.ds(pl.multiple_of(base * 4 * rows, half), half), :]
        offsets = []
        for l in range(2):
            total = offs_in[(base + l) * 4, :, :]
            for u in range(1, 4):
                total = total + offs_in[(base + l) * 4 + u, :, :]
            offsets.append(total - 1)
        sums = [acc[base + l, :, :] for l in range(2)]
        for start, size in blocks:
            scores = lax.dot_general(head_buf[slot, start:start + size, :], hidden, CONTRACT_LAST,
                                     preferred_element_type=jnp.float32)
            for l in range(2):
                low = offsets[l] & 7
                high = (offsets[l] >> 3) - start // 8
                found = jnp.zeros((SLOT_CAP, LANES), jnp.float32)
                for g in range(size // 8):
                    tile = scores[8 * g:8 * g + 8, LANES * l:LANES * l + LANES]
                    found = jnp.where(high == g, jnp.take_along_axis(tile, low, axis=0), found)
                sums[l] = sums[l] + found
        for l in range(2):
            acc[base + l, :, :] = sums[l]

        @pl.when((phase < NUM_PIECES - NUM_SLOTS) | ((phase >= NUM_PIECES) & (phase < 2 * NUM_PIECES - NUM_SLOTS)))
        def _():
            for copy in head_copies(phase + NUM_SLOTS):
                copy.start(priority=1)

        @pl.when(phase == NUM_PIECES)
        def _():
            for step in range(1, NUM_SHARDS):
                @pl.when(near(step))
                def _():
                    send_scores(step).start()

        return carry

    lax.fori_loop(0, num_phases, run_phase, 0)

    for step in range(1, NUM_SHARDS):
        @pl.when(jnp.logical_not(near(step)))
        def _():
            send_scores(step).start()
    ret_in[me, :, :] = acc[z, :, :]

    row_pos = lax.broadcasted_iota(jnp.int32, (rows, 32), 0)
    target = jnp.zeros((rows, 32), jnp.int32)
    for b in range(rows):
        target = jnp.where(row_pos == b, tgt_ref[b], target)

    def end_piece(k, carry):
        for copy in [line_send(k)] + side_sends(k) + far_sends(k):
            copy.wait_send()
        return carry

    lax.fori_loop(0, NUM_PIECES, end_piece, 0)

    def end_phase(phase, carry):
        for e in range(2):
            @pl.when(pair_base(phase) + e != z)
            def _():
                for copy in relay_sends(phase, e):
                    copy.wait_send()
            hop_send(phase, e).wait_send()
        return carry

    lax.fori_loop(0, num_phases, end_phase, 0)
    for step in range(1, NUM_SHARDS):
        send_offs(step).wait_send()
        send_scores(step).wait_send()
    for step in range(1, NUM_SHARDS):
        src = partner(step)
        pltpu.make_async_remote_copy(
            src_ref=acc.at[0], dst_ref=ret_in.at[src], send_sem=ret_send.at[step], recv_sem=ret_recv.at[src],
            device_id=device(src), device_id_type=MESH).wait_recv()

    turned[...] = jnp.zeros_like(turned)
    for q in range(4):
        owner_q, rank_q = codes[0, 8 * q:8 * q + 8, :], codes[1, 8 * q:8 * q + 8, :]
        picked = jnp.zeros((8, LANES), jnp.float32)
        for s in range(NUM_SHARDS):
            picked = jnp.where(owner_q == s, jnp.take_along_axis(ret_in[s, :, :], rank_q, axis=0), picked)
        turned[8 * q:8 * q + 8, :] = picked
    turned[...] = jnp.transpose(turned[...])
    raw = turned[pl.ds(pl.multiple_of(v * rows, rows), rows), :][:, 0:32]
    is_valid = valid_ref[...] > 0
    logits = jnp.where(is_valid, raw / TEMPERATURE, -jnp.inf)
    top = jnp.max(logits, axis=1, keepdims=True)
    log_norm = top + jnp.log(jnp.sum(jnp.exp(logits - top), axis=1, keepdims=True))
    p_ref[...] = jnp.where(is_valid, jnp.exp(logits - log_norm), 0.0)
    out_copies[0].start()
    col_pos = lax.broadcasted_iota(jnp.int32, (rows, 32), 1)
    chosen = jnp.sum(jnp.where(col_pos == target, logits, 0.0), axis=1, keepdims=True)
    turned[0:rows, :] = jnp.broadcast_to(chosen - log_norm, (rows, LANES))
    lp_ref[...] = jnp.transpose(turned[...])[0:1, 0:rows]
    out_copies[1].start()
    for copy in out_copies:
        copy.wait()


def solution(mesh):
    shard_axes = ('model', 'vocab')
    row_spec = P(('rep', 'model', 'vocab'), None)
    vec_spec = P(('rep', 'model', 'vocab'))

    def local_step(hidden, head_rows, allowed_ids, valid_mask, target_pos):
        rows, width = hidden.shape
        shard_len = head_rows.shape[0]
        depth = width // NUM_PIECES
        num_blocks = -(-shard_len // HEAD_BLOCK)
        dma = pltpu.SemaphoreType.DMA
        tile = (SLOT_CAP, LANES)
        p, lp = pl.pallas_call(
            functools.partial(kernel, shard_len, width, rows),
            out_shape=(jax.ShapeDtypeStruct((rows, 32), jnp.float32), jax.ShapeDtypeStruct((1, rows), jnp.float32)),
            in_specs=[pl.BlockSpec(memory_space=pl.ANY)] * 5,
            out_specs=(pl.BlockSpec(memory_space=pl.ANY),) * 2,
            scratch_shapes=[
                pltpu.SMEM((rows,), jnp.int32),
                pltpu.VMEM((rows, 32), jnp.int32),
                pltpu.VMEM((rows, 32), jnp.int32),
                pltpu.VMEM((rows, 32), jnp.float32),
                pltpu.VMEM((1, rows), jnp.float32),
                dma((5,)),
                pltpu.VMEM((NUM_SLOTS, shard_len, depth), jnp.bfloat16),
                pltpu.VMEM((NUM_PIECES, NUM_SHARDS * rows, depth), jnp.bfloat16),
                pltpu.VMEM((LANES, LANES), jnp.int32),
                pltpu.VMEM((LANES, LANES), jnp.float32),
                pltpu.VMEM((2, 32, LANES), jnp.int32),
                pltpu.VMEM((NUM_SHARDS,) + tile, jnp.int32),
                pltpu.VMEM((NUM_SHARDS,) + tile, jnp.int32),
                pltpu.VMEM((4,) + tile, jnp.float32),
                pltpu.VMEM((NUM_SHARDS,) + tile, jnp.float32),
                dma((NUM_SLOTS, num_blocks)), dma((NUM_PIECES,)), dma((NUM_SHARDS, NUM_PIECES)),
                dma((3, NUM_PIECES)), dma((2, NUM_PIECES)), dma((2, 2, 2 * NUM_PIECES)), dma((2, 2 * NUM_PIECES)),
                dma((NUM_SHARDS,)), dma((NUM_SHARDS,)), dma((NUM_SHARDS,)), dma((NUM_SHARDS,)),
            ],
            compiler_params=pltpu.CompilerParams(collective_id=0, has_side_effects=True, vmem_limit_bytes=67043328),
        )(target_pos, allowed_ids, valid_mask, hidden, head_rows)
        return p, lp.reshape(rows)

    return jax.shard_map(local_step, mesh=mesh, in_specs=(row_spec, P(shard_axes, None), row_spec, row_spec, vec_spec),
                         out_specs=(row_spec, vec_spec), check_vma=False)
```

```python
import functools

import jax
import jax.numpy as jnp
from jax import lax
from jax.experimental import pallas as pl
from jax.experimental.pallas import tpu as pltpu
from jax.sharding import PartitionSpec as P

TEMPERATURE = 0.5
MESH = pl.DeviceIdType.MESH
CONTRACT_LAST = (((1,), (1,)), ((), ()))
NUM_SHARDS = 16
NUM_PIECES = 8
NUM_SLOTS = 6
HEAD_BLOCK = 1008
SLOT_CAP = 8
LANES = 128
LEAD = 3


def kernel(shard_len, width, rows,
           tgt_hbm, ids_hbm, valid_hbm, hidden_ref, head_ref,
           p_hbm, lp_hbm,
           tgt_ref, ids_ref, valid_ref, p_ref, lp_ref, small_sem,
           head_buf, h_buf, square, turned, codes, offs_out, offs_in, acc, ret_in,
           head_sem, local_sem, recv_sem, own_sem, far_sem, relay_sem, hop_sem,
           offs_send, offs_recv, ret_send, ret_recv):
    depth = width // NUM_PIECES
    half = NUM_SHARDS // 2 * rows
    num_phases = 2 * NUM_PIECES
    z, v = lax.axis_index('model'), lax.axis_index('vocab')
    me = z * 4 + v
    z_near = z + 1 - 2 * lax.rem(z, 2)
    z_far = 2 * lax.rem(lax.div(z, 2) + 1, 2)
    v_other = lax.rem(v + 2, 4)
    v_sib = v + 1 - 2 * lax.rem(v, 2)
    v_sib_other = lax.rem(v_sib + 2, 4)

    def partner(step):
        return lax.rem(me + step, NUM_SHARDS)

    def device(shard):
        return {'model': lax.div(shard, 4), 'vocab': lax.rem(shard, 4)}

    barrier = pltpu.get_barrier_semaphore()
    for step in range(1, NUM_SHARDS):
        pl.semaphore_signal(barrier, inc=1, device_id=device(partner(step)), device_id_type=MESH)

    blocks = [(start, min(HEAD_BLOCK, shard_len - start)) for start in range(0, shard_len, HEAD_BLOCK)]

    def piece_of(phase):
        return lax.rem(phase + lax.div(phase, 7), 7) * (1 - lax.div(phase, 14)) + 7 * lax.div(phase, 14)

    def slot_of(phase):
        return lax.rem(phase - lax.div(phase, 15), NUM_SLOTS)

    def head_copies(phase):
        cols = pl.ds(pl.multiple_of(piece_of(phase) * depth, depth), depth)
        slot = slot_of(phase)
        return [pltpu.make_async_copy(head_ref.at[pl.ds(start, size), cols],
                                      head_buf.at[slot, pl.ds(start, size), :], head_sem.at[slot, i])
                for i, (start, size) in enumerate(blocks)]

    def block_of(shard, piece):
        return h_buf.at[piece, pl.ds(pl.multiple_of(shard * rows, rows), rows), :]

    local_copies = [pltpu.make_async_copy(hidden_ref.at[:, pl.ds(k * depth, depth)], block_of(me, k), local_sem.at[k])
                    for k in range(NUM_PIECES)]
    small_copies = [pltpu.make_async_copy(src, dst, small_sem.at[i]) for i, (src, dst) in enumerate(
        ((ids_hbm, ids_ref), (valid_hbm, valid_ref), (tgt_hbm, tgt_ref)))]
    out_copies = [pltpu.make_async_copy(src, dst, small_sem.at[3 + i]) for i, (src, dst) in enumerate(
        ((p_ref, p_hbm), (lp_ref, lp_hbm)))]
    for copy in local_copies[:LEAD] + small_copies + local_copies[LEAD:]:
        copy.start()
    for phase in range(NUM_SLOTS):
        for copy in head_copies(phase):
            copy.start(priority=1)

    pl.semaphore_wait(barrier, NUM_SHARDS - 1)

    def send_block(shard, piece, send_sem, to_z, to_v):
        return pltpu.make_async_remote_copy(
            src_ref=block_of(shard, piece), dst_ref=block_of(shard, piece), send_sem=send_sem,
            recv_sem=recv_sem.at[shard, piece], device_id={'model': to_z, 'vocab': to_v}, device_id_type=MESH)

    def arrived(shard, piece):
        send_block(shard, piece, recv_sem.at[shard, piece], z, v_sib).wait_recv()

    def line_send(k):
        return send_block(me, k, own_sem.at[0, k], z_near, v)

    def side_sends(k):
        return [send_block(me, k, own_sem.at[1, k], z, v_other), send_block(me, k, own_sem.at[2, k], z, v_sib)]

    def far_sends(k):
        return [send_block(me, k, far_sem.at[e, k], z_far + e, v) for e in range(2)]

    def send_offs(step):
        to = partner(step)
        return pltpu.make_async_remote_copy(
            src_ref=offs_out.at[to], dst_ref=offs_in.at[me], send_sem=offs_send.at[step], recv_sem=offs_recv.at[me],
            device_id=device(to), device_id_type=MESH)

    def pair_base(phase):
        far = lax.div(phase, 7) - lax.div(phase, 14) - lax.div(phase, 15)
        return 2 * lax.rem(lax.div(z, 2) + far, 2)

    def relay_sends(phase, e):
        shard, k = (pair_base(phase) + e) * 4 + v, piece_of(phase)
        return [send_block(shard, k, relay_sem.at[0, e, phase], z, v_other),
                send_block(shard, k, relay_sem.at[1, e, phase], z, v_sib)]

    def relay(phase):
        for e in range(2):
            @pl.when((phase < num_phases) & (pair_base(phase) + e != z))
            def _():
                arrived((pair_base(phase) + e) * 4 + v, piece_of(phase))
                for copy in relay_sends(phase, e):
                    copy.start()

    def hop_send(phase, e):
        return send_block((pair_base(phase) + e) * 4 + v_other, piece_of(phase), hop_sem.at[e, phase], z, v_sib)

    def hop(phase):
        @pl.when(phase < num_phases)
        def _():
            for e in range(2):
                arrived((pair_base(phase) + e) * 4 + v_other, piece_of(phase))
                hop_send(phase, e).start()

    def settle(phase):
        for e in range(2):
            arrived((pair_base(phase) + e) * 4 + v_sib, piece_of(phase))
            arrived((pair_base(phase) + e) * 4 + v_sib_other, piece_of(phase))

    def send_scores(step):
        to = partner(step)
        return pltpu.make_async_remote_copy(
            src_ref=acc.at[lax.div(to, 4)], dst_ref=ret_in.at[me], send_sem=ret_send.at[step], recv_sem=ret_recv.at[me],
            device_id=device(to), device_id_type=MESH)

    def near(step):
        return lax.div(partner(step), 8) == lax.div(me, 8)

    for k in range(LEAD):
        local_copies[k].wait()
        line_send(k).start()
        for copy in side_sends(k):
            copy.start()
    for copy in small_copies:
        copy.wait()

    square[...] = jnp.zeros_like(square)
    masked_ids = jnp.where(valid_ref[...] > 0, ids_ref[...], -1)
    for group in range(4):
        square[rows * group:rows * group + rows, 0:32] = masked_ids
    ids_t = jnp.transpose(square[...])[0:32, :]
    owner = jnp.zeros_like(ids_t)
    for s in range(1, NUM_SHARDS):
        owner = owner + jnp.where(ids_t >= s * shard_len, 1, 0)
    lane = lax.broadcasted_iota(jnp.int32, (32, LANES), 1)
    list_pos = lax.broadcasted_iota(jnp.int32, (32, LANES), 0)
    mine = (lane >= v * rows) & (lane < v * rows + rows) & (ids_t >= 0)
    owner = jnp.where(mine, owner, -1)
    offset1 = ids_t - owner * shard_len + 1
    rank = jnp.zeros_like(owner)
    for i in range(31):
        rank = rank + jnp.where((owner == owner[i:i + 1, :]) & (list_pos > i), 1, 0)
    code = jnp.where(mine, owner * SLOT_CAP + rank, -1)
    codes[0, :, :] = owner
    codes[1, :, :] = jnp.minimum(rank, SLOT_CAP - 1)
    slot_pos = lax.broadcasted_iota(jnp.int32, (SLOT_CAP, LANES), 0)
    tiles = [jnp.zeros((SLOT_CAP, LANES), jnp.int32) for _ in range(NUM_SHARDS)]
    for j in range(32):
        code_j, offset_j = code[j:j + 1, :], offset1[j:j + 1, :]
        for s in range(NUM_SHARDS):
            tiles[s] = jnp.where(code_j == slot_pos + s * SLOT_CAP, offset_j, tiles[s])
    for s in range(NUM_SHARDS):
        offs_out[s, :, :] = tiles[s]
    offs_in[me, :, :] = offs_out[me, :, :]
    acc[...] = jnp.zeros_like(acc)

    for step in range(1, NUM_SHARDS):
        @pl.when(near(step))
        def _():
            send_offs(step).start()

    for k in range(LEAD, NUM_PIECES):
        local_copies[k].wait()
    for i in range(NUM_PIECES):
        if LEAD + i < NUM_PIECES - 1:
            line_send(LEAD + i).start()
        for copy in far_sends(piece_of(7 + i)):
            copy.start()
    line_send(NUM_PIECES - 1).start()
    for step in range(1, NUM_SHARDS):
        @pl.when(jnp.logical_not(near(step)))
        def _():
            send_offs(step).start()

    for phase in range(LEAD):
        relay(phase)
        for copy in side_sends(LEAD + phase):
            copy.start()
    hop(0)

    def wait_offs(step):
        src = partner(step)
        pltpu.make_async_remote_copy(
            src_ref=offs_out.at[src], dst_ref=offs_in.at[src], send_sem=offs_send.at[step], recv_sem=offs_recv.at[src],
            device_id=device(src), device_id_type=MESH).wait_recv()

    for step in range(1, NUM_SHARDS):
        @pl.when(near(step))
        def _():
            wait_offs(step)

    def compute(phase):
        slot = slot_of(phase)
        base = pair_base(phase)
        hidden = h_buf[piece_of(phase), pl.ds(pl.multiple_of(base * 4 * rows, half), half), :]
        offsets = []
        for l in range(2):
            total = offs_in[(base + l) * 4, :, :]
            for u in range(1, 4):
                total = total + offs_in[(base + l) * 4 + u, :, :]
            offsets.append(total - 1)
        sums = [acc[base + l, :, :] for l in range(2)]
        for start, size in blocks:
            scores = lax.dot_general(head_buf[slot, start:start + size, :], hidden, CONTRACT_LAST,
                                     preferred_element_type=jnp.float32)
            for l in range(2):
                low = offsets[l] & 7
                high = (offsets[l] >> 3) - start // 8
                found = jnp.zeros((SLOT_CAP, LANES), jnp.float32)
                for g in range(size // 8):
                    tile = scores[8 * g:8 * g + 8, LANES * l:LANES * l + LANES]
                    found = jnp.where(high == g, jnp.take_along_axis(tile, low, axis=0), found)
                sums[l] = sums[l] + found
        for l in range(2):
            acc[base + l, :, :] = sums[l]

    def run_phase(phase, carry):
        @pl.when(phase < NUM_PIECES - 2 * LEAD)
        def _():
            for copy in side_sends(phase + 2 * LEAD):
                copy.start()

        relay(phase + LEAD)
        hop(phase + 1)
        settle(phase)

        @pl.when((phase < 7) | (phase == 13) | (phase == 14))
        def _():
            for copy in head_copies(phase):
                copy.wait()

        @pl.when(phase == 7)
        def _():
            for step in range(1, NUM_SHARDS):
                @pl.when(jnp.logical_not(near(step)))
                def _():
                    wait_offs(step)

        @pl.when(phase == num_phases - 1)
        def _():
            for step in range(1, NUM_SHARDS):
                @pl.when(jnp.logical_not(near(step)))
                def _():
                    send_scores(step).start()

        compute(phase)

        @pl.when((phase == 0) | (phase == 7) | (phase == 8))
        def _():
            for copy in head_copies(phase + NUM_SLOTS):
                copy.start(priority=1)

        return carry

    lax.fori_loop(0, num_phases, run_phase, 0)

    for step in range(1, NUM_SHARDS):
        @pl.when(near(step))
        def _():
            send_scores(step).start()
    ret_in[me, :, :] = acc[z, :, :]

    row_pos = lax.broadcasted_iota(jnp.int32, (rows, 32), 0)
    target = jnp.zeros((rows, 32), jnp.int32)
    for b in range(rows):
        target = jnp.where(row_pos == b, tgt_ref[b], target)

    def end_piece(k, carry):
        for copy in [line_send(k)] + side_sends(k) + far_sends(k):
            copy.wait_send()
        return carry

    lax.fori_loop(0, NUM_PIECES, end_piece, 0)

    def end_phase(phase, carry):
        for e in range(2):
            @pl.when(pair_base(phase) + e != z)
            def _():
                for copy in relay_sends(phase, e):
                    copy.wait_send()
            hop_send(phase, e).wait_send()
        return carry

    lax.fori_loop(0, num_phases, end_phase, 0)
    for step in range(1, NUM_SHARDS):
        send_offs(step).wait_send()
        send_scores(step).wait_send()
    for step in range(1, NUM_SHARDS):
        src = partner(step)
        pltpu.make_async_remote_copy(
            src_ref=acc.at[0], dst_ref=ret_in.at[src], send_sem=ret_send.at[step], recv_sem=ret_recv.at[src],
            device_id=device(src), device_id_type=MESH).wait_recv()

    turned[...] = jnp.zeros_like(turned)
    for q in range(4):
        owner_q, rank_q = codes[0, 8 * q:8 * q + 8, :], codes[1, 8 * q:8 * q + 8, :]
        picked = jnp.zeros((8, LANES), jnp.float32)
        for s in range(NUM_SHARDS):
            picked = jnp.where(owner_q == s, jnp.take_along_axis(ret_in[s, :, :], rank_q, axis=0), picked)
        turned[8 * q:8 * q + 8, :] = picked
    turned[...] = jnp.transpose(turned[...])
    raw = turned[pl.ds(pl.multiple_of(v * rows, rows), rows), :][:, 0:32]
    is_valid = valid_ref[...] > 0
    logits = jnp.where(is_valid, raw / TEMPERATURE, -jnp.inf)
    top = jnp.max(logits, axis=1, keepdims=True)
    log_norm = top + jnp.log(jnp.sum(jnp.exp(logits - top), axis=1, keepdims=True))
    p_ref[...] = jnp.where(is_valid, jnp.exp(logits - log_norm), 0.0)
    out_copies[0].start()
    col_pos = lax.broadcasted_iota(jnp.int32, (rows, 32), 1)
    chosen = jnp.sum(jnp.where(col_pos == target, logits, 0.0), axis=1, keepdims=True)
    turned[0:rows, :] = jnp.broadcast_to(chosen - log_norm, (rows, LANES))
    lp_ref[...] = jnp.transpose(turned[...])[0:1, 0:rows]
    out_copies[1].start()
    for copy in out_copies:
        copy.wait()


def solution(mesh):
    shard_axes = ('model', 'vocab')
    row_spec = P(('rep', 'model', 'vocab'), None)
    vec_spec = P(('rep', 'model', 'vocab'))

    def local_step(hidden, head_rows, allowed_ids, valid_mask, target_pos):
        rows, width = hidden.shape
        shard_len = head_rows.shape[0]
        depth = width // NUM_PIECES
        num_blocks = -(-shard_len // HEAD_BLOCK)
        dma = pltpu.SemaphoreType.DMA
        tile = (SLOT_CAP, LANES)
        p, lp = pl.pallas_call(
            functools.partial(kernel, shard_len, width, rows),
            out_shape=(jax.ShapeDtypeStruct((rows, 32), jnp.float32), jax.ShapeDtypeStruct((1, rows), jnp.float32)),
            in_specs=[pl.BlockSpec(memory_space=pl.ANY)] * 5,
            out_specs=(pl.BlockSpec(memory_space=pl.ANY),) * 2,
            scratch_shapes=[
                pltpu.SMEM((rows,), jnp.int32),
                pltpu.VMEM((rows, 32), jnp.int32),
                pltpu.VMEM((rows, 32), jnp.int32),
                pltpu.VMEM((rows, 32), jnp.float32),
                pltpu.VMEM((1, rows), jnp.float32),
                dma((5,)),
                pltpu.VMEM((NUM_SLOTS, shard_len, depth), jnp.bfloat16),
                pltpu.VMEM((NUM_PIECES, NUM_SHARDS * rows, depth), jnp.bfloat16),
                pltpu.VMEM((LANES, LANES), jnp.int32),
                pltpu.VMEM((LANES, LANES), jnp.float32),
                pltpu.VMEM((2, 32, LANES), jnp.int32),
                pltpu.VMEM((NUM_SHARDS,) + tile, jnp.int32),
                pltpu.VMEM((NUM_SHARDS,) + tile, jnp.int32),
                pltpu.VMEM((4,) + tile, jnp.float32),
                pltpu.VMEM((NUM_SHARDS,) + tile, jnp.float32),
                dma((NUM_SLOTS, num_blocks)), dma((NUM_PIECES,)), dma((NUM_SHARDS, NUM_PIECES)),
                dma((3, NUM_PIECES)), dma((2, NUM_PIECES)), dma((2, 2, 2 * NUM_PIECES)), dma((2, 2 * NUM_PIECES)),
                dma((NUM_SHARDS,)), dma((NUM_SHARDS,)), dma((NUM_SHARDS,)), dma((NUM_SHARDS,)),
            ],
            compiler_params=pltpu.CompilerParams(collective_id=0, has_side_effects=True, vmem_limit_bytes=67043328),
        )(target_pos, allowed_ids, valid_mask, hidden, head_rows)
        return p, lp.reshape(rows)

    return jax.shard_map(local_step, mesh=mesh, in_specs=(row_spec, P(shard_axes, None), row_spec, row_spec, vec_spec),
                         out_specs=(row_spec, vec_spec), check_vma=False)
```

```python
import functools

import jax
import jax.numpy as jnp
from jax import lax
from jax.experimental import pallas as pl
from jax.experimental.pallas import tpu as pltpu
from jax.sharding import PartitionSpec as P

TEMPERATURE = 0.5
MESH = pl.DeviceIdType.MESH
CONTRACT_LAST = (((1,), (1,)), ((), ()))
NUM_SHARDS = 16
NUM_PIECES = 8
NUM_SLOTS = 6
HEAD_BLOCK = 1008
SLOT_CAP = 8
LANES = 128
FAR_FIRST = 1
LEAD = 3


def kernel(shard_len, width, rows,
           tgt_hbm, ids_hbm, valid_hbm, hidden_ref, head_ref,
           p_ref, lp_ref,
           tgt_ref, ids_ref, valid_ref, small_sem,
           head_buf, h_buf, square, turned, codes, offs_out, offs_in, acc, ret_in,
           head_sem, local_sem, recv_sem, own_sem, far_sem, relay_sem, hop_sem,
           offs_send, offs_recv, ret_send, ret_recv):
    depth = width // NUM_PIECES
    half = NUM_SHARDS // 2 * rows
    num_phases = 2 * NUM_PIECES
    z, v = lax.axis_index('model'), lax.axis_index('vocab')
    me = z * 4 + v
    z_near = z + 1 - 2 * lax.rem(z, 2)
    z_far = 2 * lax.rem(lax.div(z, 2) + 1, 2)
    v_other = lax.rem(v + 2, 4)
    v_sib = v + 1 - 2 * lax.rem(v, 2)
    v_sib_other = lax.rem(v_sib + 2, 4)

    def partner(step):
        return lax.rem(me + step, NUM_SHARDS)

    def device(shard):
        return {'model': lax.div(shard, 4), 'vocab': lax.rem(shard, 4)}

    barrier = pltpu.get_barrier_semaphore()
    for step in range(1, NUM_SHARDS):
        pl.semaphore_signal(barrier, inc=1, device_id=device(partner(step)), device_id_type=MESH)

    blocks = [(start, min(HEAD_BLOCK, shard_len - start)) for start in range(0, shard_len, HEAD_BLOCK)]

    def piece_of(phase):
        return lax.rem(phase + (NUM_PIECES - NUM_SLOTS) * lax.div(phase, NUM_PIECES), NUM_PIECES)

    def head_copies(phase):
        cols = pl.ds(pl.multiple_of(piece_of(phase) * depth, depth), depth)
        slot = lax.rem(phase, NUM_SLOTS)
        return [pltpu.make_async_copy(head_ref.at[pl.ds(start, size), cols],
                                      head_buf.at[slot, pl.ds(start, size), :], head_sem.at[slot, i])
                for i, (start, size) in enumerate(blocks)]

    def block_of(shard, piece):
        return h_buf.at[piece, pl.ds(pl.multiple_of(shard * rows, rows), rows), :]

    local_copies = [pltpu.make_async_copy(hidden_ref.at[:, pl.ds(k * depth, depth)], block_of(me, k), local_sem.at[k])
                    for k in range(NUM_PIECES)]
    small_copies = [pltpu.make_async_copy(src, dst, small_sem.at[i]) for i, (src, dst) in enumerate(
        ((ids_hbm, ids_ref), (valid_hbm, valid_ref), (tgt_hbm, tgt_ref)))]
    for copy in local_copies[:LEAD] + small_copies + local_copies[LEAD:]:
        copy.start()
    for phase in range(NUM_SLOTS):
        for copy in head_copies(phase):
            copy.start(priority=1)

    pl.semaphore_wait(barrier, NUM_SHARDS - 1)

    def send_block(shard, piece, send_sem, to_z, to_v):
        return pltpu.make_async_remote_copy(
            src_ref=block_of(shard, piece), dst_ref=block_of(shard, piece), send_sem=send_sem,
            recv_sem=recv_sem.at[shard, piece], device_id={'model': to_z, 'vocab': to_v}, device_id_type=MESH)

    def arrived(shard, piece):
        send_block(shard, piece, recv_sem.at[shard, piece], z, v_sib).wait_recv()

    def line_send(k):
        return send_block(me, k, own_sem.at[0, k], z_near, v)

    def side_sends(k):
        return [send_block(me, k, own_sem.at[1, k], z, v_other), send_block(me, k, own_sem.at[2, k], z, v_sib)]

    def far_sends(k):
        return [send_block(me, k, far_sem.at[e, k], z_far + e, v) for e in range(2)]

    def send_offs(step):
        to = partner(step)
        return pltpu.make_async_remote_copy(
            src_ref=offs_out.at[to], dst_ref=offs_in.at[me], send_sem=offs_send.at[step], recv_sem=offs_recv.at[me],
            device_id=device(to), device_id_type=MESH)

    def pair_base(phase):
        return 2 * lax.rem(lax.div(z, 2) + lax.div(phase, NUM_PIECES), 2)

    def relay_sends(phase, e):
        shard, k = (pair_base(phase) + e) * 4 + v, piece_of(phase)
        return [send_block(shard, k, relay_sem.at[0, e, phase], z, v_other),
                send_block(shard, k, relay_sem.at[1, e, phase], z, v_sib)]

    def relay(phase):
        for e in range(2):
            @pl.when((phase < num_phases) & (pair_base(phase) + e != z))
            def _():
                arrived((pair_base(phase) + e) * 4 + v, piece_of(phase))
                for copy in relay_sends(phase, e):
                    copy.start()

    def hop_send(phase, e):
        return send_block((pair_base(phase) + e) * 4 + v_other, piece_of(phase), hop_sem.at[e, phase], z, v_sib)

    def hop(phase):
        @pl.when(phase < num_phases)
        def _():
            for e in range(2):
                arrived((pair_base(phase) + e) * 4 + v_other, piece_of(phase))
                hop_send(phase, e).start()

    def settle(phase):
        for e in range(2):
            arrived((pair_base(phase) + e) * 4 + v_sib, piece_of(phase))
            arrived((pair_base(phase) + e) * 4 + v_sib_other, piece_of(phase))

    def send_scores(step):
        to = partner(step)
        return pltpu.make_async_remote_copy(
            src_ref=acc.at[lax.div(to, 4)], dst_ref=ret_in.at[me], send_sem=ret_send.at[step], recv_sem=ret_recv.at[me],
            device_id=device(to), device_id_type=MESH)

    def near(step):
        return lax.div(partner(step), 8) == lax.div(me, 8)

    for k in range(LEAD):
        local_copies[k].wait()
        line_send(k).start()
        for copy in side_sends(k):
            copy.start()
    for copy in small_copies:
        copy.wait()

    square[...] = jnp.zeros_like(square)
    masked_ids = jnp.where(valid_ref[...] > 0, ids_ref[...], -1)
    for group in range(4):
        square[rows * group:rows * group + rows, 0:32] = masked_ids
    ids_t = jnp.transpose(square[...])[0:32, :]
    owner = jnp.zeros_like(ids_t)
    for s in range(1, NUM_SHARDS):
        owner = owner + jnp.where(ids_t >= s * shard_len, 1, 0)
    lane = lax.broadcasted_iota(jnp.int32, (32, LANES), 1)
    list_pos = lax.broadcasted_iota(jnp.int32, (32, LANES), 0)
    mine = (lane >= v * rows) & (lane < v * rows + rows) & (ids_t >= 0)
    owner = jnp.where(mine, owner, -1)
    offset1 = ids_t - owner * shard_len + 1
    rank = jnp.zeros_like(owner)
    for i in range(31):
        rank = rank + jnp.where((owner == owner[i:i + 1, :]) & (list_pos > i), 1, 0)
    code = jnp.where(mine, owner * SLOT_CAP + rank, -1)
    codes[0, :, :] = owner
    codes[1, :, :] = jnp.minimum(rank, SLOT_CAP - 1)
    slot_pos = lax.broadcasted_iota(jnp.int32, (SLOT_CAP, LANES), 0)
    tiles = [jnp.zeros((SLOT_CAP, LANES), jnp.int32) for _ in range(NUM_SHARDS)]
    for j in range(32):
        code_j, offset_j = code[j:j + 1, :], offset1[j:j + 1, :]
        for s in range(NUM_SHARDS):
            tiles[s] = jnp.where(code_j == slot_pos + s * SLOT_CAP, offset_j, tiles[s])
    for s in range(NUM_SHARDS):
        offs_out[s, :, :] = tiles[s]
    offs_in[me, :, :] = offs_out[me, :, :]
    acc[...] = jnp.zeros_like(acc)

    for step in range(1, NUM_SHARDS):
        send_offs(step).start()
    for k in range(LEAD, NUM_PIECES):
        local_copies[k].wait()
        line_send(k).start()
    for phase in range(LEAD):
        relay(phase)
        for copy in side_sends(LEAD + phase):
            copy.start()
    hop(0)
    for i in range(FAR_FIRST):
        for copy in far_sends(piece_of(NUM_PIECES + i)):
            copy.start()

    def wait_offs(step):
        src = partner(step)
        pltpu.make_async_remote_copy(
            src_ref=offs_out.at[src], dst_ref=offs_in.at[src], send_sem=offs_send.at[step], recv_sem=offs_recv.at[src],
            device_id=device(src), device_id_type=MESH).wait_recv()

    for step in range(1, NUM_SHARDS):
        wait_offs(step)

    def run_phase(phase, carry):
        @pl.when(phase < NUM_PIECES - FAR_FIRST)
        def _():
            for copy in far_sends(piece_of(phase + NUM_PIECES + FAR_FIRST)):
                copy.start()

        relay(phase + LEAD)

        @pl.when(phase < NUM_PIECES - 2 * LEAD)
        def _():
            for copy in side_sends(phase + 2 * LEAD):
                copy.start()

        hop(phase + 1)
        settle(phase)

        @pl.when((phase < NUM_PIECES) | (phase >= NUM_PIECES + NUM_SLOTS))
        def _():
            for copy in head_copies(phase):
                copy.wait()

        slot = lax.rem(phase, NUM_SLOTS)
        base = pair_base(phase)
        hidden = h_buf[piece_of(phase), pl.ds(pl.multiple_of(base * 4 * rows, half), half), :]
        offsets = []
        for l in range(2):
            total = offs_in[(base + l) * 4, :, :]
            for u in range(1, 4):
                total = total + offs_in[(base + l) * 4 + u, :, :]
            offsets.append(total - 1)
        sums = [acc[base + l, :, :] for l in range(2)]
        for start, size in blocks:
            scores = lax.dot_general(head_buf[slot, start:start + size, :], hidden, CONTRACT_LAST,
                                     preferred_element_type=jnp.float32)
            for l in range(2):
                low = offsets[l] & 7
                high = (offsets[l] >> 3) - start // 8
                found = jnp.zeros((SLOT_CAP, LANES), jnp.float32)
                for g in range(size // 8):
                    tile = scores[8 * g:8 * g + 8, LANES * l:LANES * l + LANES]
                    found = jnp.where(high == g, jnp.take_along_axis(tile, low, axis=0), found)
                sums[l] = sums[l] + found
        for l in range(2):
            acc[base + l, :, :] = sums[l]

        @pl.when((phase < NUM_PIECES - NUM_SLOTS) | ((phase >= NUM_PIECES) & (phase < 2 * NUM_PIECES - NUM_SLOTS)))
        def _():
            for copy in head_copies(phase + NUM_SLOTS):
                copy.start(priority=1)

        @pl.when(phase == NUM_PIECES)
        def _():
            for step in range(1, NUM_SHARDS):
                @pl.when(near(step))
                def _():
                    send_scores(step).start()

        return carry

    lax.fori_loop(0, num_phases, run_phase, 0)

    for step in range(1, NUM_SHARDS):
        @pl.when(jnp.logical_not(near(step)))
        def _():
            send_scores(step).start()
    ret_in[me, :, :] = acc[z, :, :]

    row_pos = lax.broadcasted_iota(jnp.int32, (rows, 32), 0)
    target = jnp.zeros((rows, 32), jnp.int32)
    for b in range(rows):
        target = jnp.where(row_pos == b, tgt_ref[b], target)

    def end_piece(k, carry):
        for copy in [line_send(k)] + side_sends(k) + far_sends(k):
            copy.wait_send()
        return carry

    lax.fori_loop(0, NUM_PIECES, end_piece, 0)

    def end_phase(phase, carry):
        for e in range(2):
            @pl.when(pair_base(phase) + e != z)
            def _():
                for copy in relay_sends(phase, e):
                    copy.wait_send()
            hop_send(phase, e).wait_send()
        return carry

    lax.fori_loop(0, num_phases, end_phase, 0)
    for step in range(1, NUM_SHARDS):
        send_offs(step).wait_send()
        send_scores(step).wait_send()
    for step in range(1, NUM_SHARDS):
        src = partner(step)
        pltpu.make_async_remote_copy(
            src_ref=acc.at[0], dst_ref=ret_in.at[src], send_sem=ret_send.at[step], recv_sem=ret_recv.at[src],
            device_id=device(src), device_id_type=MESH).wait_recv()

    turned[...] = jnp.zeros_like(turned)
    for q in range(4):
        owner_q, rank_q = codes[0, 8 * q:8 * q + 8, :], codes[1, 8 * q:8 * q + 8, :]
        picked = jnp.zeros((8, LANES), jnp.float32)
        for s in range(NUM_SHARDS):
            picked = jnp.where(owner_q == s, jnp.take_along_axis(ret_in[s, :, :], rank_q, axis=0), picked)
        turned[8 * q:8 * q + 8, :] = picked
    turned[...] = jnp.transpose(turned[...])
    raw = turned[pl.ds(pl.multiple_of(v * rows, rows), rows), :][:, 0:32]
    is_valid = valid_ref[...] > 0
    logits = jnp.where(is_valid, raw / TEMPERATURE, -jnp.inf)
    top = jnp.max(logits, axis=1, keepdims=True)
    log_norm = top + jnp.log(jnp.sum(jnp.exp(logits - top), axis=1, keepdims=True))
    p_ref[...] = jnp.where(is_valid, jnp.exp(logits - log_norm), 0.0)
    col_pos = lax.broadcasted_iota(jnp.int32, (rows, 32), 1)
    chosen = jnp.sum(jnp.where(col_pos == target, logits, 0.0), axis=1, keepdims=True)
    turned[0:rows, :] = jnp.broadcast_to(chosen - log_norm, (rows, LANES))
    lp_ref[...] = jnp.transpose(turned[...])[0:1, 0:rows]


def solution(mesh):
    shard_axes = ('model', 'vocab')
    row_spec = P(('rep', 'model', 'vocab'), None)
    vec_spec = P(('rep', 'model', 'vocab'))

    def local_step(hidden, head_rows, allowed_ids, valid_mask, target_pos):
        rows, width = hidden.shape
        shard_len = head_rows.shape[0]
        depth = width // NUM_PIECES
        num_blocks = -(-shard_len // HEAD_BLOCK)
        dma = pltpu.SemaphoreType.DMA
        tile = (SLOT_CAP, LANES)
        p, lp = pl.pallas_call(
            functools.partial(kernel, shard_len, width, rows),
            out_shape=(pltpu.VMEM((rows, 32), jnp.float32), pltpu.VMEM((1, rows), jnp.float32)),
            in_specs=[pl.BlockSpec(memory_space=pl.ANY)] * 5,
            out_specs=(pl.BlockSpec(memory_space=pltpu.VMEM),) * 2,
            scratch_shapes=[
                pltpu.SMEM((rows,), jnp.int32),
                pltpu.VMEM((rows, 32), jnp.int32),
                pltpu.VMEM((rows, 32), jnp.int32),
                dma((3,)),
                pltpu.VMEM((NUM_SLOTS, shard_len, depth), jnp.bfloat16),
                pltpu.VMEM((NUM_PIECES, NUM_SHARDS * rows, depth), jnp.bfloat16),
                pltpu.VMEM((LANES, LANES), jnp.int32),
                pltpu.VMEM((LANES, LANES), jnp.float32),
                pltpu.VMEM((2, 32, LANES), jnp.int32),
                pltpu.VMEM((NUM_SHARDS,) + tile, jnp.int32),
                pltpu.VMEM((NUM_SHARDS,) + tile, jnp.int32),
                pltpu.VMEM((4,) + tile, jnp.float32),
                pltpu.VMEM((NUM_SHARDS,) + tile, jnp.float32),
                dma((NUM_SLOTS, num_blocks)), dma((NUM_PIECES,)), dma((NUM_SHARDS, NUM_PIECES)),
                dma((3, NUM_PIECES)), dma((2, NUM_PIECES)), dma((2, 2, 2 * NUM_PIECES)), dma((2, 2 * NUM_PIECES)),
                dma((NUM_SHARDS,)), dma((NUM_SHARDS,)), dma((NUM_SHARDS,)), dma((NUM_SHARDS,)),
            ],
            compiler_params=pltpu.CompilerParams(collective_id=0, has_side_effects=True, vmem_limit_bytes=62 * 2**20),
        )(target_pos, allowed_ids, valid_mask, hidden, head_rows)
        return p, lp.reshape(rows)

    return jax.shard_map(local_step, mesh=mesh, in_specs=(row_spec, P(shard_axes, None), row_spec, row_spec, vec_spec),
                         out_specs=(row_spec, vec_spec), check_vma=False)
```

```python
import functools

import jax
import jax.numpy as jnp
from jax import lax
from jax.experimental import pallas as pl
from jax.experimental.pallas import tpu as pltpu
from jax.sharding import PartitionSpec as P

TEMPERATURE = 0.5
MESH = pl.DeviceIdType.MESH
CONTRACT_LAST = (((1,), (1,)), ((), ()))
NUM_SHARDS = 16
NUM_PIECES = 8
NUM_SLOTS = 6
HEAD_BLOCK = 1008
HEAD_LOAD = 2016
SLOT_CAP = 8
LANES = 128
FAR_FIRST = 1
LEAD = 3


def kernel(shard_len, width, rows,
           tgt_hbm, ids_hbm, valid_hbm, hidden_ref, head_ref,
           p_ref, lp_ref,
           tgt_ref, ids_ref, valid_ref, small_sem,
           head_buf, h_buf, square, turned, codes, offs_out, offs_in, acc, ret_in,
           head_sem, local_sem, recv_sem, own_sem, far_sem, relay_sem, hop_sem,
           offs_send, offs_recv, ret_send, ret_recv):
    depth = width // NUM_PIECES
    half = NUM_SHARDS // 2 * rows
    num_phases = 2 * NUM_PIECES
    z, v = lax.axis_index('model'), lax.axis_index('vocab')
    me = z * 4 + v
    z_near = z + 1 - 2 * lax.rem(z, 2)
    z_far = 2 * lax.rem(lax.div(z, 2) + 1, 2)
    v_other = lax.rem(v + 2, 4)
    v_sib = v + 1 - 2 * lax.rem(v, 2)
    v_sib_other = lax.rem(v_sib + 2, 4)

    def partner(step):
        return lax.rem(me + step, NUM_SHARDS)

    def device(shard):
        return {'model': lax.div(shard, 4), 'vocab': lax.rem(shard, 4)}

    barrier = pltpu.get_barrier_semaphore()
    for step in range(1, NUM_SHARDS):
        pl.semaphore_signal(barrier, inc=1, device_id=device(partner(step)), device_id_type=MESH)

    blocks = [(start, min(HEAD_BLOCK, shard_len - start)) for start in range(0, shard_len, HEAD_BLOCK)]
    loads = [(start, min(HEAD_LOAD, shard_len - start)) for start in range(0, shard_len, HEAD_LOAD)]

    def piece_of(phase):
        return lax.rem(phase + (NUM_PIECES - NUM_SLOTS) * lax.div(phase, NUM_PIECES), NUM_PIECES)

    def head_copies(phase):
        cols = pl.ds(pl.multiple_of(piece_of(phase) * depth, depth), depth)
        slot = lax.rem(phase, NUM_SLOTS)
        return [pltpu.make_async_copy(head_ref.at[pl.ds(start, size), cols],
                                      head_buf.at[slot, pl.ds(start, size), :], head_sem.at[slot, i])
                for i, (start, size) in enumerate(loads)]

    def block_of(shard, piece):
        return h_buf.at[piece, pl.ds(pl.multiple_of(shard * rows, rows), rows), :]

    local_copies = [pltpu.make_async_copy(hidden_ref.at[:, pl.ds(k * depth, depth)], block_of(me, k), local_sem.at[k])
                    for k in range(NUM_PIECES)]
    small_copies = [pltpu.make_async_copy(src, dst, small_sem.at[i]) for i, (src, dst) in enumerate(
        ((ids_hbm, ids_ref), (valid_hbm, valid_ref), (tgt_hbm, tgt_ref)))]
    for copy in local_copies[:LEAD] + small_copies + local_copies[LEAD:]:
        copy.start()
    for phase in range(NUM_SLOTS):
        for copy in head_copies(phase):
            copy.start(priority=1)

    pl.semaphore_wait(barrier, NUM_SHARDS - 1)

    def send_block(shard, piece, send_sem, to_z, to_v):
        return pltpu.make_async_remote_copy(
            src_ref=block_of(shard, piece), dst_ref=block_of(shard, piece), send_sem=send_sem,
            recv_sem=recv_sem.at[shard, piece], device_id={'model': to_z, 'vocab': to_v}, device_id_type=MESH)

    def arrived(shard, piece):
        send_block(shard, piece, recv_sem.at[shard, piece], z, v_sib).wait_recv()

    def line_send(k):
        return send_block(me, k, own_sem.at[0, k], z_near, v)

    def side_sends(k):
        return [send_block(me, k, own_sem.at[1, k], z, v_other), send_block(me, k, own_sem.at[2, k], z, v_sib)]

    def far_sends(k):
        return [send_block(me, k, far_sem.at[e, k], z_far + e, v) for e in range(2)]

    def send_offs(step):
        to = partner(step)
        return pltpu.make_async_remote_copy(
            src_ref=offs_out.at[to], dst_ref=offs_in.at[me], send_sem=offs_send.at[step], recv_sem=offs_recv.at[me],
            device_id=device(to), device_id_type=MESH)

    def pair_base(phase):
        return 2 * lax.rem(lax.div(z, 2) + lax.div(phase, NUM_PIECES), 2)

    def relay_sends(phase, e):
        shard, k = (pair_base(phase) + e) * 4 + v, piece_of(phase)
        return [send_block(shard, k, relay_sem.at[0, e, phase], z, v_other),
                send_block(shard, k, relay_sem.at[1, e, phase], z, v_sib)]

    def relay(phase):
        for e in range(2):
            @pl.when((phase < num_phases) & (pair_base(phase) + e != z))
            def _():
                arrived((pair_base(phase) + e) * 4 + v, piece_of(phase))
                for copy in relay_sends(phase, e):
                    copy.start()

    def hop_send(phase, e):
        return send_block((pair_base(phase) + e) * 4 + v_other, piece_of(phase), hop_sem.at[e, phase], z, v_sib)

    def hop(phase):
        @pl.when(phase < num_phases)
        def _():
            for e in range(2):
                arrived((pair_base(phase) + e) * 4 + v_other, piece_of(phase))
                hop_send(phase, e).start()

    def settle(phase):
        for e in range(2):
            arrived((pair_base(phase) + e) * 4 + v_sib, piece_of(phase))
            arrived((pair_base(phase) + e) * 4 + v_sib_other, piece_of(phase))

    def send_scores(step):
        to = partner(step)
        return pltpu.make_async_remote_copy(
            src_ref=acc.at[lax.div(to, 4)], dst_ref=ret_in.at[me], send_sem=ret_send.at[step], recv_sem=ret_recv.at[me],
            device_id=device(to), device_id_type=MESH)

    def near(step):
        return lax.div(partner(step), 8) == lax.div(me, 8)

    for k in range(LEAD):
        local_copies[k].wait()
        line_send(k).start()
        for copy in side_sends(k):
            copy.start()
    for copy in small_copies:
        copy.wait()

    square[...] = jnp.zeros_like(square)
    masked_ids = jnp.where(valid_ref[...] > 0, ids_ref[...], -1)
    for group in range(4):
        square[rows * group:rows * group + rows, 0:32] = masked_ids
    ids_t = jnp.transpose(square[...])[0:32, :]
    owner = jnp.zeros_like(ids_t)
    for s in range(1, NUM_SHARDS):
        owner = owner + jnp.where(ids_t >= s * shard_len, 1, 0)
    lane = lax.broadcasted_iota(jnp.int32, (32, LANES), 1)
    list_pos = lax.broadcasted_iota(jnp.int32, (32, LANES), 0)
    mine = (lane >= v * rows) & (lane < v * rows + rows) & (ids_t >= 0)
    owner = jnp.where(mine, owner, -1)
    offset1 = ids_t - owner * shard_len + 1
    rank = jnp.zeros_like(owner)
    for i in range(31):
        rank = rank + jnp.where((owner == owner[i:i + 1, :]) & (list_pos > i), 1, 0)
    code = jnp.where(mine, owner * SLOT_CAP + rank, -1)
    codes[0, :, :] = owner
    codes[1, :, :] = jnp.minimum(rank, SLOT_CAP - 1)
    slot_pos = lax.broadcasted_iota(jnp.int32, (SLOT_CAP, LANES), 0)
    tiles = [jnp.zeros((SLOT_CAP, LANES), jnp.int32) for _ in range(NUM_SHARDS)]
    for j in range(32):
        code_j, offset_j = code[j:j + 1, :], offset1[j:j + 1, :]
        for s in range(NUM_SHARDS):
            tiles[s] = jnp.where(code_j == slot_pos + s * SLOT_CAP, offset_j, tiles[s])
    for s in range(NUM_SHARDS):
        offs_out[s, :, :] = tiles[s]
    offs_in[me, :, :] = offs_out[me, :, :]
    acc[...] = jnp.zeros_like(acc)

    for step in range(1, NUM_SHARDS):
        send_offs(step).start()
    for k in range(LEAD, NUM_PIECES):
        local_copies[k].wait()
        line_send(k).start()
    for phase in range(LEAD):
        relay(phase)
    for phase in range(LEAD):
        for copy in side_sends(LEAD + phase):
            copy.start()
    hop(0)
    for i in range(FAR_FIRST):
        for copy in far_sends(piece_of(NUM_PIECES + i)):
            copy.start()

    def wait_offs(step):
        src = partner(step)
        pltpu.make_async_remote_copy(
            src_ref=offs_out.at[src], dst_ref=offs_in.at[src], send_sem=offs_send.at[step], recv_sem=offs_recv.at[src],
            device_id=device(src), device_id_type=MESH).wait_recv()

    for step in range(1, NUM_SHARDS):
        wait_offs(step)

    def run_phase(phase, carry):
        @pl.when(phase < NUM_PIECES - FAR_FIRST)
        def _():
            for copy in far_sends(piece_of(phase + NUM_PIECES + FAR_FIRST)):
                copy.start()

        relay(phase + LEAD)

        @pl.when(phase < NUM_PIECES - 2 * LEAD)
        def _():
            for copy in side_sends(phase + 2 * LEAD):
                copy.start()

        hop(phase + 1)
        settle(phase)

        @pl.when((phase < NUM_PIECES) | (phase >= NUM_PIECES + NUM_SLOTS))
        def _():
            for copy in head_copies(phase):
                copy.wait()

        slot = lax.rem(phase, NUM_SLOTS)
        base = pair_base(phase)
        hidden = h_buf[piece_of(phase), pl.ds(pl.multiple_of(base * 4 * rows, half), half), :]
        offsets = []
        for l in range(2):
            total = offs_in[(base + l) * 4, :, :]
            for u in range(1, 4):
                total = total + offs_in[(base + l) * 4 + u, :, :]
            offsets.append(total - 1)
        sums = [acc[base + l, :, :] for l in range(2)]
        for start, size in blocks:
            scores = lax.dot_general(head_buf[slot, start:start + size, :], hidden, CONTRACT_LAST,
                                     preferred_element_type=jnp.float32)
            for l in range(2):
                low = offsets[l] & 7
                high = (offsets[l] >> 3) - start // 8
                found = jnp.zeros((SLOT_CAP, LANES), jnp.float32)
                for g in range(size // 8):
                    tile = scores[8 * g:8 * g + 8, LANES * l:LANES * l + LANES]
                    found = jnp.where(high == g, jnp.take_along_axis(tile, low, axis=0), found)
                sums[l] = sums[l] + found
        for l in range(2):
            acc[base + l, :, :] = sums[l]

        @pl.when((phase < NUM_PIECES - NUM_SLOTS) | ((phase >= NUM_PIECES) & (phase < 2 * NUM_PIECES - NUM_SLOTS)))
        def _():
            for copy in head_copies(phase + NUM_SLOTS):
                copy.start(priority=1)

        @pl.when(phase == NUM_PIECES)
        def _():
            for step in range(1, NUM_SHARDS):
                @pl.when(near(step))
                def _():
                    send_scores(step).start()

        return carry

    lax.fori_loop(0, num_phases, run_phase, 0)

    for step in range(1, NUM_SHARDS):
        @pl.when(jnp.logical_not(near(step)))
        def _():
            send_scores(step).start()
    ret_in[me, :, :] = acc[z, :, :]

    row_pos = lax.broadcasted_iota(jnp.int32, (rows, 32), 0)
    target = jnp.zeros((rows, 32), jnp.int32)
    for b in range(rows):
        target = jnp.where(row_pos == b, tgt_ref[b], target)

    def end_piece(k, carry):
        for copy in [line_send(k)] + side_sends(k) + far_sends(k):
            copy.wait_send()
        return carry

    lax.fori_loop(0, NUM_PIECES, end_piece, 0)

    def end_phase(phase, carry):
        for e in range(2):
            @pl.when(pair_base(phase) + e != z)
            def _():
                for copy in relay_sends(phase, e):
                    copy.wait_send()
            hop_send(phase, e).wait_send()
        return carry

    lax.fori_loop(0, num_phases, end_phase, 0)
    for step in range(1, NUM_SHARDS):
        send_offs(step).wait_send()
        send_scores(step).wait_send()
    for step in range(1, NUM_SHARDS):
        src = partner(step)
        pltpu.make_async_remote_copy(
            src_ref=acc.at[0], dst_ref=ret_in.at[src], send_sem=ret_send.at[step], recv_sem=ret_recv.at[src],
            device_id=device(src), device_id_type=MESH).wait_recv()

    turned[...] = jnp.zeros_like(turned)
    for q in range(4):
        owner_q, rank_q = codes[0, 8 * q:8 * q + 8, :], codes[1, 8 * q:8 * q + 8, :]
        picked = jnp.zeros((8, LANES), jnp.float32)
        for s in range(NUM_SHARDS):
            picked = jnp.where(owner_q == s, jnp.take_along_axis(ret_in[s, :, :], rank_q, axis=0), picked)
        turned[8 * q:8 * q + 8, :] = picked
    turned[...] = jnp.transpose(turned[...])
    raw = turned[pl.ds(pl.multiple_of(v * rows, rows), rows), :][:, 0:32]
    is_valid = valid_ref[...] > 0
    logits = jnp.where(is_valid, raw / TEMPERATURE, -jnp.inf)
    top = jnp.max(logits, axis=1, keepdims=True)
    log_norm = top + jnp.log(jnp.sum(jnp.exp(logits - top), axis=1, keepdims=True))
    p_ref[...] = jnp.where(is_valid, jnp.exp(logits - log_norm), 0.0)
    col_pos = lax.broadcasted_iota(jnp.int32, (rows, 32), 1)
    chosen = jnp.sum(jnp.where(col_pos == target, logits, 0.0), axis=1, keepdims=True)
    turned[0:rows, :] = jnp.broadcast_to(chosen - log_norm, (rows, LANES))
    lp_ref[...] = jnp.transpose(turned[...])[0:1, 0:rows]


def solution(mesh):
    shard_axes = ('model', 'vocab')
    row_spec = P(('rep', 'model', 'vocab'), None)
    vec_spec = P(('rep', 'model', 'vocab'))

    def local_step(hidden, head_rows, allowed_ids, valid_mask, target_pos):
        rows, width = hidden.shape
        shard_len = head_rows.shape[0]
        depth = width // NUM_PIECES
        num_blocks = -(-shard_len // HEAD_BLOCK)
        dma = pltpu.SemaphoreType.DMA
        tile = (SLOT_CAP, LANES)
        p, lp = pl.pallas_call(
            functools.partial(kernel, shard_len, width, rows),
            out_shape=(pltpu.VMEM((rows, 32), jnp.float32), pltpu.VMEM((1, rows), jnp.float32)),
            in_specs=[pl.BlockSpec(memory_space=pl.ANY)] * 5,
            out_specs=(pl.BlockSpec(memory_space=pltpu.VMEM),) * 2,
            scratch_shapes=[
                pltpu.SMEM((rows,), jnp.int32),
                pltpu.VMEM((rows, 32), jnp.int32),
                pltpu.VMEM((rows, 32), jnp.int32),
                dma((3,)),
                pltpu.VMEM((NUM_SLOTS, shard_len, depth), jnp.bfloat16),
                pltpu.VMEM((NUM_PIECES, NUM_SHARDS * rows, depth), jnp.bfloat16),
                pltpu.VMEM((LANES, LANES), jnp.int32),
                pltpu.VMEM((LANES, LANES), jnp.float32),
                pltpu.VMEM((2, 32, LANES), jnp.int32),
                pltpu.VMEM((NUM_SHARDS,) + tile, jnp.int32),
                pltpu.VMEM((NUM_SHARDS,) + tile, jnp.int32),
                pltpu.VMEM((4,) + tile, jnp.float32),
                pltpu.VMEM((NUM_SHARDS,) + tile, jnp.float32),
                dma((NUM_SLOTS, num_blocks)), dma((NUM_PIECES,)), dma((NUM_SHARDS, NUM_PIECES)),
                dma((3, NUM_PIECES)), dma((2, NUM_PIECES)), dma((2, 2, 2 * NUM_PIECES)), dma((2, 2 * NUM_PIECES)),
                dma((NUM_SHARDS,)), dma((NUM_SHARDS,)), dma((NUM_SHARDS,)), dma((NUM_SHARDS,)),
            ],
            compiler_params=pltpu.CompilerParams(collective_id=0, has_side_effects=True, vmem_limit_bytes=62 * 2**20),
        )(target_pos, allowed_ids, valid_mask, hidden, head_rows)
        return p, lp.reshape(rows)

    return jax.shard_map(local_step, mesh=mesh, in_specs=(row_spec, P(shard_axes, None), row_spec, row_spec, vec_spec),
                         out_specs=(row_spec, vec_spec), check_vma=False)
```
